128 devices in a mesh: rows: 16 (over x, z), cols: 8 (over y, core).
Axes of the slice: x: 4, y: 4, z: 4, core: 2. Of those that a mesh axis runs over, the one named last changes fastest.
Arguments:
- bag_index: int32 [2048, 128], P(('rows', 'cols')), may hold values from 0 to 1048575, as said below
- bag_length: int32 [2048, 4], P(('rows', 'cols')), may hold values from 1 to 32
- emb_tables: float32 [4, 1048576, 128], P(None, ('rows', 'cols')), may hold values from -0.6 to 0.6
- dense_feats: float32 [2048, 128], P(('rows', 'cols')), may hold values from -6 to 6
- w_dense: float32 [128, 1024], replicated, may hold values from -0.5 to 0.5
- w_pair: float32 [10, 1024], replicated, may hold values from -0.5 to 0.5
- top_bias: float32 [1024], replicated, may hold values from -3 to 3
Outputs:
- pooled: float32 [2048, 4, 128], P(('rows', 'cols'))
- top_hidden: float32 [2048, 1024], P(('rows', 'cols'))
The draws below stay inside these ranges and needn't reach their ends.
Inputs may be any that keep to these rules, and one draw needn't show every extreme that they name: `bag_length`: slots at or past a bag's length are ignored, whatever they hold. `bag_index`: device d holds rows d * 8192 to (d + 1) * 8192 - 1 of every table; among the 2048 slots (live or not) of the samples of one device, at most 32 hold rows of any one device, and in every draw some device's rows receive exactly 32 slots from every device.
All inputs are finite; a program needn't handle non-finite values.
Results may differ from the reference program's by a relative error of at most 0.0001.
Values sent between devices are 32-bit elements; how exact they have to be, the bound alone decides.
No kernel may reach another device: no remote copies, remote signals or barrier semaphores. Data moves between devices by JAX's collectives and lax.ppermute only.
A program may use at most 128 MiB of HBM per device.

```python
import jax
import jax.numpy as jnp
from jax import lax

E = 128
ROWS_DEV = 8192
NT = 4
L = 32
H = 1024
SAMP_DEV = 16
B = 2048
VOCAB = 1048576
PAIRS = 10


def draw_bag_index(key, part):
    ndevices = B // SAMP_DEV
    slots = SAMP_DEV * NT * L
    capacity = 2 * slots // ndevices
    total = ndevices * capacity
    token_owner = jnp.arange(total, dtype=jnp.int32) // capacity
    key_weight, key_common, key_blocks = jax.random.split(key, 3)
    weight = jax.random.randint(key_weight, (ndevices,), 0, 4, dtype=jnp.int32) * 512
    common_hot = jax.random.randint(key_common, (), 0, ndevices, dtype=jnp.int32)

    def one_block(block_key):
        key_own, key_score, key_order, key_first, key_second = jax.random.split(block_key, 5)
        own_hot = jax.random.randint(key_own, (), 0, ndevices, dtype=jnp.int32)
        forced = jnp.where((token_owner == common_hot) | (token_owner == own_hot), 4096, 0).astype(jnp.int32)
        score = jax.random.randint(key_score, (total,), 0, 1024, dtype=jnp.int32) + weight[token_owner] + forced
        score = score * total + jnp.arange(total, dtype=jnp.int32)
        unused, chosen = lax.top_k(score, slots)
        order = jax.random.permutation(key_order, slots)
        owners = token_owner[chosen[order]]
        first_draw = jax.random.randint(key_first, (slots,), 0, ROWS_DEV, dtype=jnp.int32)
        second_draw = jax.random.randint(key_second, (slots,), 1, ROWS_DEV + 1, dtype=jnp.int32)
        local = first_draw * second_draw // ROWS_DEV
        return (owners * ROWS_DEV + local).reshape(SAMP_DEV, NT * L)
    block_keys = jax.random.split(key_blocks, ndevices)
    return jax.vmap(one_block)(block_keys).reshape(B, NT * L).astype(jnp.int32)


def touch_ends(drawn, own_key, least, largest):
    dims = drawn.shape
    spot = [jax.random.randint(jax.random.fold_in(own_key, axis), (), 0, dims[axis]) for axis in range(len(dims))]
    drawn = drawn.at[tuple(spot)].set(least)
    longest = dims.index(max(dims))
    spot[longest] = (spot[longest] + 1) % dims[longest]
    return drawn.at[tuple(spot)].set(largest)


def block_scale(own_key, extent, cuts, smallest, largest):
    factor_of = 1.0
    for axis_at, parts in cuts:
        draws = jax.random.uniform(jax.random.fold_in(jax.random.fold_in(own_key, 6), axis_at), (parts,), jnp.float32, smallest / len(cuts), largest / len(cuts))
        factor_of = factor_of * jnp.repeat(jnp.exp(draws), extent[axis_at] // parts).reshape((-1,) + (1,) * (len(extent) - 1 - axis_at))
    return factor_of


def normal_values(stream_key, shape, spread, bound, cuts=(), held_as=jnp.bfloat16):
    drawn = spread * jax.random.normal(stream_key, shape, jnp.float32)
    if cuts:
        drawn = drawn * block_scale(stream_key, shape, cuts, -0.22, 0.18)
    return jnp.clip(drawn, -bound, bound).astype(held_as)


def setup_inputs(seed: int = 0) -> dict:
    seeds = jax.random.split(jax.random.key(seed), 8)
    return {
        "bag_index": draw_bag_index(jax.random.fold_in(seeds[7], 71), 0),
        "bag_length": touch_ends(jax.random.randint(seeds[1], (B, NT), 1, L + 1), jax.random.fold_in(seeds[1], 1), 1, L).astype(jnp.int32),
        "emb_tables": normal_values(seeds[2], (NT, VOCAB, E), 0.1, 0.6, ((1, 128),), jnp.float32),
        "dense_feats": normal_values(seeds[3], (B, E), 1.0, 6.0, ((0, 128),), jnp.float32),
        "w_dense": normal_values(seeds[4], (E, H), (E + PAIRS) ** -0.5, 0.5, (), jnp.float32),
        "w_pair": normal_values(seeds[5], (PAIRS, H), (E + PAIRS) ** -0.5, 0.5, (), jnp.float32),
        "top_bias": normal_values(seeds[6], (H,), 0.5, 3.0, (), jnp.float32),
    }


def interact(dense_feats, pooled, w_dense, w_pair, top_bias):
    feats = [dense_feats] + [pooled[:, t, :] for t in range(NT)]
    pair_list = []
    for first in range(NT + 1):
        for second in range(first + 1, NT + 1):
            pair_list.append(jnp.sum(feats[first] * feats[second], axis=-1))
    pair_dots = jnp.stack(pair_list, axis=1)
    hidden = jnp.dot(dense_feats, w_dense, precision=lax.Precision.HIGHEST, preferred_element_type=jnp.float32)
    hidden = hidden + jnp.dot(pair_dots, w_pair, precision=lax.Precision.HIGHEST, preferred_element_type=jnp.float32)
    return jnp.maximum(hidden + top_bias, 0.0)


def reference(bag_index, bag_length, emb_tables, dense_feats, w_dense, w_pair, top_bias):
    position = jnp.arange(L, dtype=jnp.int32)
    pieces = []
    for table in range(NT):
        ids = bag_index[:, table * L:(table + 1) * L]
        live = position[None, :] < bag_length[:, table:table + 1]
        picked = jnp.take(emb_tables[table], ids, axis=0)
        pieces.append(jnp.sum(jnp.where(live[:, :, None], picked, 0.0), axis=1))
    pooled = jnp.stack(pieces, axis=1)
    return pooled, interact(dense_feats, pooled, w_dense, w_pair, top_bias)
```

```python
import jax
import jax.numpy as jnp
from jax import lax
from jax.experimental import pallas as pl
from jax.experimental.pallas import tpu as pltpu
from jax.sharding import PartitionSpec as P

NT = 4
L = 32
LANES = 128


def route_kernel(idx_ref, len_ref, code_ref, meta_ref, *, local_rows, devices, capacity):
    samples = idx_ref.shape[0]
    shift = local_rows.bit_length() - 1
    ids = idx_ref[...]
    target = ids >> shift
    lane = lax.broadcasted_iota(jnp.int32, (samples, LANES), 1)
    table = lane // L
    code = table * local_rows + (ids & (local_rows - 1))
    length = jnp.zeros((samples, LANES), jnp.int32)
    for t in range(NT):
        length = jnp.where(table == t, len_ref[:, t : t + 1], length)
    row = lax.broadcasted_iota(jnp.int32, (samples, LANES), 0)
    meta = jnp.where(lane - table * L < length, table * samples + row + 1, 0)
    high = (code >> 8).astype(jnp.float32)
    low = (code & 255).astype(jnp.float32)
    meta = meta.astype(jnp.float32)

    owner = lax.broadcasted_iota(jnp.int32, (devices, LANES), 0)
    hots = [
        jnp.where(owner == target[i : i + 1, :], 1.0, 0.0) for i in range(samples)
    ]
    earlier = lax.broadcasted_iota(jnp.int32, (LANES, 2 * LANES), 0)
    later = lax.broadcasted_iota(jnp.int32, (LANES, 2 * LANES), 1)
    counter = jnp.where(earlier < later, 1.0, 0.0).astype(jnp.bfloat16)
    hot_stack = jnp.concatenate(hots, axis=0).astype(jnp.bfloat16)
    counts = jnp.dot(hot_stack, counter, preferred_element_type=jnp.float32)
    place = lax.broadcasted_iota(jnp.int32, (capacity, LANES), 0).astype(jnp.float32)
    before = jnp.zeros((devices, LANES), jnp.float32)
    pieces = []
    for i in range(samples):
        block = counts[i * devices : (i + 1) * devices]
        rank = jnp.sum(hots[i] * (block[:, :LANES] + before), axis=0, keepdims=True)
        before = before + block[:, LANES:]
        here = place == rank
        pieces.append(
            jnp.concatenate(
                [
                    jnp.where(here, high[i : i + 1, :], 0.0),
                    jnp.where(here, low[i : i + 1, :], 0.0),
                    jnp.where(here, meta[i : i + 1, :], 0.0),
                ],
                axis=0,
            ).astype(jnp.bfloat16)
        )
    hot_wide = jnp.concatenate([h.astype(jnp.bfloat16) for h in hots], axis=1)
    values = jnp.concatenate(pieces, axis=1)
    box = lax.dot_general(
        hot_wide, values, (((1,), (1,)), ((), ())), preferred_element_type=jnp.float32
    )
    code_ref[...] = (
        box[:, :capacity] * 256.0 + box[:, capacity : 2 * capacity]
    ).astype(jnp.int32)
    meta_ref[...] = box[:, 2 * capacity :].astype(jnp.int32)


def gather_kernel(ids_ref, table_ref, out_ref, *, capacity):
    def one(src, carry):
        for c in range(capacity):
            out_ref[src * capacity + c, 0] = table_ref[ids_ref[src, c], 0]
        return carry

    lax.fori_loop(0, ids_ref.shape[0], one, 0)


def pool_kernel(rows_ref, meta_ref, dense_ref, base_ref, wpair_ref, pooled_ref, hidden_ref):
    groups = meta_ref.shape[0]
    samples = dense_ref.shape[0]
    bags = NT * samples
    bag = lax.broadcasted_iota(jnp.int32, (bags, LANES), 0) + 1
    total = jnp.zeros((bags, 2 * LANES), jnp.float32)
    rows = rows_ref[...]
    top = rows.astype(jnp.bfloat16)
    rest = (rows - top.astype(jnp.float32)).astype(jnp.bfloat16)
    select = jnp.concatenate(
        [jnp.where(meta_ref[g : g + 1, :] == bag, 1.0, 0.0) for g in range(groups)], axis=1
    ).astype(jnp.bfloat16)
    total = jnp.dot(
        select, jnp.concatenate([top, rest], axis=1), preferred_element_type=jnp.float32
    )
    pooled = total[:, :LANES] + total[:, LANES:]
    feats = [dense_ref[...]] + [pooled[t * samples : (t + 1) * samples] for t in range(NT)]
    for t in range(NT):
        pooled_ref[pl.ds(t, samples, stride=NT), :] = feats[t + 1]
    hidden = base_ref[...]
    k = 0
    for first in range(NT + 1):
        for second in range(first + 1, NT + 1):
            dots = jnp.sum(feats[first] * feats[second], axis=-1, keepdims=True)
            hidden = hidden + dots * wpair_ref[k : k + 1, :]
            k += 1
    hidden_ref[...] = jnp.maximum(hidden, 0.0)


def shards(bag_index, bag_length, emb_tables, dense_feats, w_dense, w_pair, top_bias):
    samples = bag_index.shape[0]
    local_rows = emb_tables.shape[1]
    width = emb_tables.shape[2]
    devices = lax.axis_size("rows") * lax.axis_size("cols")
    slots = samples * NT * L
    capacity = 2 * slots // devices
    units = w_dense.shape[1]
    places = devices * capacity

    import functools

    codes, meta = pl.pallas_call(
        functools.partial(
            route_kernel, local_rows=local_rows, devices=devices, capacity=capacity
        ),
        out_shape=(
            jax.ShapeDtypeStruct((devices, capacity), jnp.int32),
            jax.ShapeDtypeStruct((devices, capacity), jnp.int32),
        ),
        name="route",
    )(bag_index, bag_length)
    wanted = lax.all_to_all(codes, ("rows", "cols"), split_axis=0, concat_axis=0, tiled=True)
    found = pl.pallas_call(
        functools.partial(gather_kernel, capacity=capacity),
        out_shape=jax.ShapeDtypeStruct((places, 1, width), jnp.float32),
        in_specs=[
            pl.BlockSpec(memory_space=pltpu.SMEM),
            pl.BlockSpec(memory_space=pltpu.VMEM),
        ],
        out_specs=pl.BlockSpec(memory_space=pltpu.VMEM),
        compiler_params=pltpu.CompilerParams(vmem_limit_bytes=40 * 2**20),
        name="fetch",
    )(wanted, emb_tables.reshape(NT * local_rows, 1, width))
    fetched = lax.all_to_all(
        found.reshape(devices, capacity, width),
        ("rows", "cols"),
        split_axis=0,
        concat_axis=0,
        tiled=True,
    )
    base = jnp.dot(
        dense_feats, w_dense, precision=lax.Precision.HIGHEST, preferred_element_type=jnp.float32
    ) + top_bias
    pooled, hidden = pl.pallas_call(
        pool_kernel,
        out_shape=(
            jax.ShapeDtypeStruct((samples * NT, width), jnp.float32),
            jax.ShapeDtypeStruct((samples, units), jnp.float32),
        ),
        compiler_params=pltpu.CompilerParams(vmem_limit_bytes=24 * 2**20),
        name="pool",
    )(
        fetched.reshape(places, width),
        meta.reshape(places // LANES, LANES),
        dense_feats,
        base,
        w_pair,
    )
    return pooled.reshape(samples, NT, width), hidden


def solution(mesh):
    in_specs = (
        P(("rows", "cols"), None),
        P(("rows", "cols"), None),
        P(None, ("rows", "cols"), None),
        P(("rows", "cols"), None),
        P(),
        P(),
        P(),
    )
    out_specs = (P(("rows", "cols"), None, None), P(("rows", "cols"), None))
    return jax.shard_map(shards, mesh=mesh, in_specs=in_specs, out_specs=out_specs, check_vma=False)
```

```python
import functools

import jax
import jax.numpy as jnp
from jax import lax
from jax.experimental import pallas as pl
from jax.experimental.pallas import tpu as pltpu
from jax.sharding import PartitionSpec as P

NT = 4
L = 32
LANES = 128
BOTH_LANES = (((1,), (1,)), ((), ()))


def iota(shape, axis):
    return lax.broadcasted_iota(jnp.int32, shape, axis)


def route_kernel(idx_ref, code_ref, rank_ref, *, local_rows, devices, capacity):
    samples = idx_ref.shape[0]
    ids = idx_ref[...]
    target = ids >> (local_rows.bit_length() - 1)
    code = iota((samples, LANES), 1) // L * local_rows + (ids & (local_rows - 1))
    high = (code >> 8).astype(jnp.float32)
    low = (code & 255).astype(jnp.float32)

    owner = iota((devices, LANES), 0)
    hots = [jnp.where(owner == target[i : i + 1, :], 1.0, 0.0) for i in range(samples)]
    hot_stack = jnp.concatenate(hots, axis=0).astype(jnp.bfloat16)
    counter = jnp.where(
        iota((LANES, 2 * LANES), 0) < iota((LANES, 2 * LANES), 1), 1.0, 0.0
    ).astype(jnp.bfloat16)
    counts = jnp.dot(hot_stack, counter, preferred_element_type=jnp.float32)
    place = iota((capacity, LANES), 0).astype(jnp.float32)
    before = jnp.zeros((devices, LANES), jnp.float32)
    pieces = []
    for i in range(samples):
        block = counts[i * devices : (i + 1) * devices]
        rank = jnp.sum(hots[i] * (block[:, :LANES] + before), axis=0, keepdims=True)
        rank_ref[i : i + 1, :] = rank
        before = before + block[:, LANES:]
        here = place == rank
        pieces.append(
            jnp.concatenate(
                [
                    jnp.where(here, high[i : i + 1, :], 0.0),
                    jnp.where(here, low[i : i + 1, :], 0.0),
                ],
                axis=0,
            ).astype(jnp.bfloat16)
        )
    hot_wide = jnp.concatenate([h.astype(jnp.bfloat16) for h in hots], axis=1)
    values = jnp.concatenate(pieces, axis=1)
    box = lax.dot_general(hot_wide, values, BOTH_LANES, preferred_element_type=jnp.float32)
    code_ref[...] = (box[:, :capacity] * 256.0 + box[:, capacity:]).astype(jnp.int32)


def fetch_kernel(
    wanted_ref, idx_ref, rank_ref, len_ref, dense_ref, wdense_ref, bias_ref, table_ref,
    out_ref, select_ref, base_ref, ids_ref, sem,
    *, local_rows, capacity,
):
    copy = pltpu.make_async_copy(wanted_ref, ids_ref, sem)
    copy.start()
    samples = idx_ref.shape[0]
    target = idx_ref[...] >> (local_rows.bit_length() - 1)
    per_row = LANES // capacity
    groups = select_ref.shape[1] // LANES
    group = target // per_row
    key = (target - group * per_row) * capacity + rank_ref[...].astype(jnp.int32)
    spread = jnp.where(iota((NT, LANES), 1) // L == iota((NT, LANES), 0), 1.0, 0.0)
    length = lax.dot_general(
        len_ref[...].astype(jnp.float32).astype(jnp.bfloat16),
        spread.astype(jnp.bfloat16),
        (((0,), (0,)), ((), ())),
        preferred_element_type=jnp.float32,
    ).astype(jnp.int32)
    lane = iota((samples, LANES), 1)
    bag = lane // L * samples + iota((samples, LANES), 0) + 1
    bag = jnp.where(lane % L < length, bag, 0).astype(jnp.float32)
    left, right = [], []
    for i in range(samples):
        left.append(jnp.where(iota((groups, LANES), 0) == group[i : i + 1, :], 1.0, 0.0))
        right.append(
            jnp.where(iota((LANES, LANES), 0) == key[i : i + 1, :], bag[i : i + 1, :], 0.0)
        )
    bags = lax.dot_general(
        jnp.concatenate(left, axis=1).astype(jnp.bfloat16),
        jnp.concatenate(right, axis=1).astype(jnp.bfloat16),
        BOTH_LANES,
        preferred_element_type=jnp.float32,
    ).astype(jnp.int32)
    own = iota((NT * samples, LANES), 0) + 1
    for g in range(groups):
        select_ref[:, g * LANES : (g + 1) * LANES] = jnp.where(
            bags[g : g + 1, :] == own, 1.0, 0.0
        ).astype(jnp.bfloat16)
    base_ref[...] = (
        jnp.dot(
            dense_ref[...],
            wdense_ref[...],
            precision=lax.Precision.HIGHEST,
            preferred_element_type=jnp.float32,
        )
        + bias_ref[...]
    )
    copy.wait()

    def one(src, carry):
        for c in range(capacity):
            out_ref[src * capacity + c, 0] = table_ref[ids_ref[src, c], 0]
        return carry

    for src in range(ids_ref.shape[0]):
        one(src, 0)


def pool_kernel(rows_ref, select_ref, dense_ref, base_ref, wpair_ref, pooled_ref, hidden_ref):
    samples = dense_ref.shape[0]
    rows = rows_ref[...]
    top = rows.astype(jnp.bfloat16)
    rest = (rows - top.astype(jnp.float32)).astype(jnp.bfloat16)
    total = jnp.dot(
        select_ref[...],
        jnp.concatenate([top, rest], axis=1),
        preferred_element_type=jnp.float32,
    )
    pooled = total[:, :LANES] + total[:, LANES:]
    feats = [dense_ref[...]] + [pooled[t * samples : (t + 1) * samples] for t in range(NT)]
    for t in range(NT):
        pooled_ref[pl.ds(t, samples, stride=NT), :] = feats[t + 1]
    hidden = base_ref[...]
    k = 0
    for first in range(NT + 1):
        for second in range(first + 1, NT + 1):
            dots = jnp.sum(feats[first] * feats[second], axis=-1, keepdims=True)
            hidden = hidden + dots * wpair_ref[k : k + 1, :]
            k += 1
    hidden_ref[...] = jnp.maximum(hidden, 0.0)


def shards(bag_index, bag_length, emb_tables, dense_feats, w_dense, w_pair, top_bias):
    samples = bag_index.shape[0]
    local_rows = emb_tables.shape[1]
    width = emb_tables.shape[2]
    devices = lax.axis_size("rows") * lax.axis_size("cols")
    slots = samples * NT * L
    capacity = 2 * slots // devices
    units = w_dense.shape[1]
    places = devices * capacity
    vmem = pl.BlockSpec(memory_space=pltpu.VMEM)

    codes, rank = pl.pallas_call(
        functools.partial(
            route_kernel, local_rows=local_rows, devices=devices, capacity=capacity
        ),
        out_shape=(
            jax.ShapeDtypeStruct((devices, capacity), jnp.int32),
            pltpu.VMEM((samples, LANES), jnp.float32),
        ),
        compiler_params=pltpu.CompilerParams(vmem_limit_bytes=8 * 2**20),
        cost_estimate=pl.CostEstimate(flops=10**10, bytes_accessed=10**8, transcendentals=0),
        name="route",
    )(bag_index)
    wanted = lax.all_to_all(codes, ("rows", "cols"), split_axis=0, concat_axis=0, tiled=True)
    found, select, base = pl.pallas_call(
        functools.partial(fetch_kernel, local_rows=local_rows, capacity=capacity),
        out_shape=(
            pltpu.VMEM((places, 1, width), jnp.float32),
            pltpu.VMEM((samples * NT, places), jnp.bfloat16),
            pltpu.VMEM((samples, units), jnp.float32),
        ),
        in_specs=[vmem] * 8,
        out_specs=(vmem, vmem, vmem),
        scratch_shapes=[pltpu.SMEM((devices, capacity), jnp.int32), pltpu.SemaphoreType.DMA],
        compiler_params=pltpu.CompilerParams(vmem_limit_bytes=8 * 2**20),
        name="fetch",
    )(
        wanted,
        bag_index,
        rank,
        bag_length.T,
        dense_feats,
        w_dense,
        top_bias.reshape(1, units),
        emb_tables.reshape(NT * local_rows, 1, width),
    )
    fetched = lax.all_to_all(
        found.reshape(devices, capacity, width),
        ("rows", "cols"),
        split_axis=0,
        concat_axis=0,
        tiled=True,
    )
    pooled, hidden = pl.pallas_call(
        pool_kernel,
        out_shape=(
            jax.ShapeDtypeStruct((samples * NT, width), jnp.float32),
            jax.ShapeDtypeStruct((samples, units), jnp.float32),
        ),
        compiler_params=pltpu.CompilerParams(vmem_limit_bytes=16 * 2**20),
        name="pool",
    )(fetched.reshape(places, width), select, dense_feats, base, w_pair)
    return pooled.reshape(samples, NT, width), hidden


def solution(mesh):
    in_specs = (
        P(("rows", "cols"), None),
        P(("rows", "cols"), None),
        P(None, ("rows", "cols"), None),
        P(("rows", "cols"), None),
        P(),
        P(),
        P(),
    )
    out_specs = (P(("rows", "cols"), None, None), P(("rows", "cols"), None))
    return jax.shard_map(shards, mesh=mesh, in_specs=in_specs, out_specs=out_specs, check_vma=False)
```

```python
import functools

import jax
import jax.numpy as jnp
from jax import lax
from jax.experimental import pallas as pl
from jax.experimental.pallas import tpu as pltpu
from jax.sharding import PartitionSpec as P

NT = 4
L = 32
LANES = 128
SMALL = 26
BOTH_LANES = (((1,), (1,)), ((), ()))


def iota(shape, axis):
    return lax.broadcasted_iota(jnp.int32, shape, axis)


def ones_where(mask):
    return jnp.where(mask, 1.0, 0.0)


def route_kernel(idx_ref, len_ref, message_ref, place_ref, *, local_rows, devices, capacity, small):
    samples = idx_ref.shape[0]
    ids = idx_ref[...]
    lane = iota((samples, LANES), 1)
    spread = ones_where(iota((NT, LANES), 1) // L == iota((NT, LANES), 0)).astype(jnp.bfloat16)
    length = lax.dot_general(
        len_ref[...].astype(jnp.float32).astype(jnp.bfloat16),
        spread,
        (((0,), (0,)), ((), ())),
        preferred_element_type=jnp.float32,
    ).astype(jnp.int32)
    target = jnp.where(lane % L < length, ids >> (local_rows.bit_length() - 1), -1)
    code = lane // L * local_rows + (ids & (local_rows - 1))
    high = (code & -256).astype(jnp.float32)
    low = (code & 255).astype(jnp.float32)

    owner = iota((devices, LANES), 0)
    hots = [ones_where(owner == target[i : i + 1, :]) for i in range(samples)]
    row = iota((LANES, LANES), 0)
    column = iota((LANES, LANES), 1)
    ones = jnp.ones((LANES, LANES), jnp.float32)
    counter = jnp.concatenate(
        [
            ones_where(row < column),
            ones,
            ones_where((row < column) & (row // L == column // L)),
        ],
        axis=1,
    ).astype(jnp.bfloat16)
    counts = jnp.dot(
        jnp.concatenate(hots, axis=0).astype(jnp.bfloat16),
        counter,
        preferred_element_type=jnp.float32,
    )
    firsts = [
        jnp.where(counts[i * devices : (i + 1) * devices, 2 * LANES :] == 0.0, hots[i], 0.0)
        for i in range(samples)
    ]
    groups = jnp.dot(
        jnp.concatenate(firsts, axis=0).astype(jnp.bfloat16),
        jnp.concatenate([ones_where(row <= column), ones], axis=1).astype(jnp.bfloat16),
        preferred_element_type=jnp.float32,
    )
    slot = iota((capacity, LANES), 0).astype(jnp.float32)
    before = jnp.zeros((devices, LANES), jnp.float32)
    groups_before = jnp.zeros((devices, LANES), jnp.float32)
    uppers, lowers = [], []
    for i in range(samples):
        block = counts[i * devices : (i + 1) * devices]
        group = groups[i * devices : (i + 1) * devices]
        rank = jnp.sum(hots[i] * (block[:, :LANES] + before), axis=0, keepdims=True)
        which = jnp.sum(hots[i] * (group[:, :LANES] + groups_before), axis=0, keepdims=True)
        first = jnp.sum(firsts[i], axis=0, keepdims=True)
        before = before + block[:, LANES : 2 * LANES]
        groups_before = groups_before + group[:, LANES:]
        here = slot == rank
        uppers.append(
            jnp.concatenate(
                [jnp.where(here, high[i : i + 1, :], 0.0), jnp.where(here, which, 0.0)], axis=0
            ).astype(jnp.bfloat16)
        )
        lowers.append(jnp.where(here, low[i : i + 1, :], 0.0).astype(jnp.bfloat16))
        own = target[i : i + 1, :] * small + which.astype(jnp.int32) - 1
        place_ref[i : i + 1, :] = jnp.where((first > 0.0) & (which <= small), own, -1)
    hot_wide = jnp.concatenate([h.astype(jnp.bfloat16) for h in hots], axis=1)
    slots = samples * LANES
    upper = jnp.concatenate(
        [jnp.concatenate(uppers, axis=1), jnp.zeros((LANES - 2 * capacity, slots), jnp.bfloat16)],
        axis=0,
    )
    lower = jnp.concatenate(
        [jnp.concatenate(lowers, axis=1), jnp.zeros((LANES - capacity, slots), jnp.bfloat16)],
        axis=0,
    )
    box = lax.dot_general(
        hot_wide, upper, BOTH_LANES, preferred_element_type=jnp.float32
    ) + lax.dot_general(hot_wide, lower, BOTH_LANES, preferred_element_type=jnp.float32)
    need = jnp.max(groups_before, axis=0, keepdims=True)
    message_ref[...] = jnp.where(
        iota((devices, LANES), 1) < 2 * capacity, box, need
    ).astype(jnp.int32)


def fetch_kernel(
    wanted_ref, place_ref, dense_ref, wdense_ref, bias_ref, table_ref,
    out_ref, select_ref, base_ref, need_ref, ids_ref, key_ref, rows_ref, sem,
    *, capacity, small, rolled,
):
    copy = pltpu.make_async_copy(wanted_ref, ids_ref, sem)
    copy.start()
    devices = wanted_ref.shape[0]
    samples = place_ref.shape[0]
    per_block = LANES // capacity
    blocks = devices // per_block
    rows_out = per_block * small

    wanted = wanted_ref[...]
    need = jnp.max(
        jnp.where(iota((devices, LANES), 1) < 2 * capacity, 0, wanted), axis=0, keepdims=True
    )
    need_ref[...] = jnp.broadcast_to(need, need_ref.shape)
    keys = jnp.zeros((blocks, LANES), jnp.int32)
    for k in range(per_block):
        which = wanted_ref[pl.ds(k, blocks, stride=per_block), :]
        which = pltpu.roll(which, (k - 1) * capacity % LANES, axis=1)
        which = jnp.where((which > 0) & (which <= small), which + (k * small - 1), -1)
        keys = jnp.where(iota((blocks, LANES), 1) // capacity == k, which, keys)
    for b in range(blocks):
        key_ref[b] = keys[b : b + 1, :]

    place = place_ref[...]
    parts = select_ref.shape[1] // LANES
    padded = -(-parts // 8) * 8
    part = place >> 7
    spot = place & (LANES - 1)
    lane = iota((1, LANES), 1)
    left, right = [], []
    for i in range(samples):
        bag = (lane // L * samples + (i + 1)).astype(jnp.float32)
        left.append(ones_where(iota((padded, LANES), 0) == part[i : i + 1, :]))
        right.append(jnp.where(iota((LANES, LANES), 0) == spot[i : i + 1, :], bag, 0.0))
    bags = lax.dot_general(
        jnp.concatenate(left, axis=1).astype(jnp.bfloat16),
        jnp.concatenate(right, axis=1).astype(jnp.bfloat16),
        BOTH_LANES,
        preferred_element_type=jnp.float32,
    ).astype(jnp.int32)
    own = iota((NT * samples, LANES), 0) + 1
    for g in range(parts):
        select_ref[:, g * LANES : (g + 1) * LANES] = ones_where(bags[g : g + 1, :] == own).astype(
            jnp.bfloat16
        )
    base_ref[...] = (
        jnp.dot(
            dense_ref[...],
            wdense_ref[...],
            precision=lax.Precision.HIGHEST,
            preferred_element_type=jnp.float32,
        )
        + bias_ref[...]
    )
    copy.wait()

    def one(b, hold):
        for k in range(per_block):
            for c in range(capacity):
                at = hold + k * capacity + c
                rows_ref[at : at + 1, :] = table_ref[ids_ref[b * per_block + k, c]]
        rows = rows_ref[hold : hold + LANES, :]
        top = rows.astype(jnp.bfloat16)
        rest = (rows - top.astype(jnp.float32)).astype(jnp.bfloat16)
        gather = ones_where(iota((rows_out, LANES), 0) == key_ref[b]).astype(jnp.bfloat16)
        sums = jnp.dot(
            gather, jnp.concatenate([top, rest], axis=1), preferred_element_type=jnp.float32
        )
        start = b * rows_out if isinstance(b, int) else pl.multiple_of(b * rows_out, 8)
        out_ref[pl.ds(start, rows_out), :] = sums[:, :LANES] + sums[:, LANES:]

    if rolled:
        lax.fori_loop(0, blocks, lambda b, carry: (one(b, 0), carry)[1], 0)
    else:
        for b in range(blocks):
            one(b, b * LANES)


def pool_kernel(
    rows_ref, select_ref, dense_ref, base_ref, wpair_ref, need_ref,
    pooled_ref, hidden_ref, over_ref,
    *, small,
):
    over_ref[0] = (jnp.max(need_ref[...]) > small).astype(jnp.int32)
    samples = dense_ref.shape[0]
    rows = rows_ref[...]
    top = rows.astype(jnp.bfloat16)
    rest = (rows - top.astype(jnp.float32)).astype(jnp.bfloat16)
    total = jnp.dot(
        select_ref[...],
        jnp.concatenate([top, rest], axis=1),
        preferred_element_type=jnp.float32,
    )
    pooled = total[:, :LANES] + total[:, LANES:]
    feats = [dense_ref[...]] + [pooled[t * samples : (t + 1) * samples] for t in range(NT)]
    for t in range(NT):
        pooled_ref[pl.ds(t, samples, stride=NT), :] = feats[t + 1]
    hidden = base_ref[...]
    k = 0
    for first in range(NT + 1):
        for second in range(first + 1, NT + 1):
            dots = jnp.sum(feats[first] * feats[second], axis=-1, keepdims=True)
            hidden = hidden + dots * wpair_ref[k : k + 1, :]
            k += 1
    hidden_ref[...] = jnp.maximum(hidden, 0.0)


def exchange(
    bag_index, bag_length, emb_tables, dense_feats, w_dense, w_pair, top_bias, *, small, rolled
):
    samples = bag_index.shape[0]
    local_rows = emb_tables.shape[1]
    width = emb_tables.shape[2]
    devices = lax.axis_size("rows") * lax.axis_size("cols")
    capacity = 2 * samples * NT * L // devices
    units = w_dense.shape[1]
    places = devices * small
    vmem = pl.BlockSpec(memory_space=pltpu.VMEM)

    message, place = pl.pallas_call(
        functools.partial(
            route_kernel, local_rows=local_rows, devices=devices, capacity=capacity, small=small
        ),
        out_shape=(
            pltpu.VMEM((devices, LANES), jnp.int32),
            pltpu.VMEM((samples, LANES), jnp.int32),
        ),
        compiler_params=pltpu.CompilerParams(vmem_limit_bytes=16 * 2**20),
        cost_estimate=pl.CostEstimate(flops=10**10, bytes_accessed=10**8, transcendentals=0),
        name="route",
    )(bag_index, bag_length.T)
    wanted = lax.all_to_all(message, ("rows", "cols"), split_axis=0, concat_axis=0, tiled=True)
    found, select, base, need = pl.pallas_call(
        functools.partial(fetch_kernel, capacity=capacity, small=small, rolled=rolled),
        out_shape=(
            pltpu.VMEM((places, width), jnp.float32),
            pltpu.VMEM((samples * NT, places), jnp.bfloat16),
            pltpu.VMEM((samples, units), jnp.float32),
            pltpu.VMEM((8, LANES), jnp.int32),
        ),
        in_specs=[vmem] * 6,
        out_specs=(vmem,) * 4,
        scratch_shapes=[
            pltpu.SMEM((devices, LANES), jnp.int32),
            pltpu.VMEM((devices * capacity // LANES, 1, LANES), jnp.int32),
            pltpu.VMEM((LANES if rolled else devices * capacity, width), jnp.float32),
            pltpu.SemaphoreType.DMA,
        ],
        compiler_params=pltpu.CompilerParams(vmem_limit_bytes=(40 if rolled else 16) * 2**20),
        name="fetch",
    )(
        wanted,
        place,
        dense_feats,
        w_dense,
        top_bias.reshape(1, units),
        emb_tables.reshape(NT * local_rows, 1, width),
    )
    fetched = lax.all_to_all(
        found.reshape(places, 1, width),
        ("rows", "cols"),
        split_axis=0,
        concat_axis=0,
        tiled=True,
    )
    return pl.pallas_call(
        functools.partial(pool_kernel, small=small),
        out_shape=(
            jax.ShapeDtypeStruct((samples * NT, width), jnp.float32),
            jax.ShapeDtypeStruct((samples, units), jnp.float32),
            jax.ShapeDtypeStruct((1,), jnp.int32),
        ),
        in_specs=[vmem] * 6,
        out_specs=(vmem, vmem, pl.BlockSpec(memory_space=pltpu.SMEM)),
        compiler_params=pltpu.CompilerParams(vmem_limit_bytes=16 * 2**20),
        name="pool",
    )(fetched.reshape(places, width), select, dense_feats, base, w_pair, need)


def shards(*args):
    samples = args[0].shape[0]
    capacity = 2 * samples * NT * L // (lax.axis_size("rows") * lax.axis_size("cols"))
    pooled, hidden, over = exchange(*args, small=SMALL, rolled=False)
    args = lax.optimization_barrier((*args, over))[:-1]
    pooled, hidden = lax.cond(
        over[0] > 0,
        lambda p, h: exchange(*args, small=capacity, rolled=True)[:2],
        lambda p, h: (p, h),
        pooled,
        hidden,
    )
    return pooled.reshape(samples, NT, -1), hidden


def solution(mesh):
    in_specs = (
        P(("rows", "cols"), None),
        P(("rows", "cols"), None),
        P(None, ("rows", "cols"), None),
        P(("rows", "cols"), None),
        P(),
        P(),
        P(),
    )
    out_specs = (P(("rows", "cols"), None, None), P(("rows", "cols"), None))
    return jax.shard_map(shards, mesh=mesh, in_specs=in_specs, out_specs=out_specs, check_vma=False)
```

```python
import functools

import jax
import jax.numpy as jnp
from jax import lax
from jax.experimental import pallas as pl
from jax.experimental.pallas import tpu as pltpu
from jax.sharding import PartitionSpec as P

NT = 4
L = 32
LANES = 128
SMALL = 25
BLOCK = 8
CHUNKS = 2
LAG = 0
BOTH_LANES = (((1,), (1,)), ((), ()))


def iota(shape, axis):
    return lax.broadcasted_iota(jnp.int32, shape, axis)


def ones_where(mask):
    return jnp.where(mask, 1.0, 0.0)


def route_kernel(idx_ref, len_ref, message_ref, place_ref, *, local_rows, devices, capacity, small):
    samples = idx_ref.shape[0]
    ids = idx_ref[...]
    lane = iota((samples, LANES), 1)
    spread = ones_where(iota((NT, LANES), 1) // L == iota((NT, LANES), 0)).astype(jnp.bfloat16)
    length = lax.dot_general(
        len_ref[...].astype(jnp.float32).astype(jnp.bfloat16),
        spread,
        (((0,), (0,)), ((), ())),
        preferred_element_type=jnp.float32,
    ).astype(jnp.int32)
    target = jnp.where(lane % L < length, ids >> (local_rows.bit_length() - 1), -1)
    code = lane // L * local_rows + (ids & (local_rows - 1))
    high = (code & -256).astype(jnp.float32)
    low = (code & 255).astype(jnp.float32)

    repeat = jnp.zeros((samples, LANES), jnp.int32)
    for k in range(1, L):
        same = (pltpu.roll(target, k, axis=1) == target) & (lane % L >= k)
        repeat = jnp.where(same, 1, repeat)
    leader = jnp.where(repeat == 0, target, -1)

    owner = iota((devices, LANES), 0)
    row = iota((2 * LANES, LANES), 0)
    column = iota((2 * LANES, LANES), 1)
    whole = row >= LANES

    def running(marks, mask):
        seen = jnp.zeros((devices, LANES), jnp.float32)
        stack = []
        for mark in marks:
            stack.append(jnp.concatenate([mark, seen], axis=1).astype(jnp.bfloat16))
            seen = seen + mark
        counter = ones_where(mask | whole).astype(jnp.bfloat16)
        return jnp.dot(
            jnp.concatenate(stack, axis=0), counter, preferred_element_type=jnp.float32
        ), seen

    hots = [ones_where(owner == target[i : i + 1, :]) for i in range(samples)]
    firsts = [ones_where(owner == leader[i : i + 1, :]) for i in range(samples)]
    counts, _ = running(hots, row < column)
    groups, seen = running(firsts, row <= column)
    slot = iota((capacity, LANES), 0).astype(jnp.float32)
    uppers, lowers = [], []
    for i in range(samples):
        block = counts[i * devices : (i + 1) * devices]
        group = groups[i * devices : (i + 1) * devices]
        rank = jnp.sum(hots[i] * block, axis=0, keepdims=True)
        which = jnp.sum(hots[i] * group, axis=0, keepdims=True)
        here = slot == rank
        uppers.append(
            jnp.concatenate(
                [jnp.where(here, high[i : i + 1, :], 0.0), jnp.where(here, which, 0.0)], axis=0
            ).astype(jnp.bfloat16)
        )
        lowers.append(jnp.where(here, low[i : i + 1, :], 0.0).astype(jnp.bfloat16))
        own = target[i : i + 1, :] * small + which.astype(jnp.int32) - 1
        place_ref[i : i + 1, :] = jnp.where(
            (leader[i : i + 1, :] >= 0) & (which <= small), own, -1
        )
    hot_wide = jnp.concatenate([h.astype(jnp.bfloat16) for h in hots], axis=1)
    slots = samples * LANES
    upper = jnp.concatenate(
        [jnp.concatenate(uppers, axis=1), jnp.zeros((LANES - 2 * capacity, slots), jnp.bfloat16)],
        axis=0,
    )
    lower = jnp.concatenate(
        [jnp.concatenate(lowers, axis=1), jnp.zeros((LANES - capacity, slots), jnp.bfloat16)],
        axis=0,
    )
    box = lax.dot_general(
        hot_wide, upper, BOTH_LANES, preferred_element_type=jnp.float32
    ) + lax.dot_general(hot_wide, lower, BOTH_LANES, preferred_element_type=jnp.float32)
    need = jnp.max(jnp.sum(seen, axis=1, keepdims=True), axis=0, keepdims=True)
    message_ref[...] = jnp.where(
        iota((devices, LANES), 1) < 2 * capacity, box, need
    ).astype(jnp.int32)


def fetch_kernel(
    wanted_ref, place_ref, dense_ref, wdense_ref, bias_ref, table_ref,
    out_ref, select_ref, base_ref, need_ref, ids_ref, key_ref, rows_ref, sems,
    *, capacity, small, rolled,
):
    devices = wanted_ref.shape[0]
    chunk = devices // CHUNKS
    copies = [
        pltpu.make_async_copy(
            wanted_ref.at[pl.ds(k * chunk, chunk)], ids_ref.at[pl.ds(k * chunk, chunk)], sems.at[k]
        )
        for k in range(CHUNKS)
    ]
    for copy in copies:
        copy.start()
    samples = place_ref.shape[0]
    wide = BLOCK * capacity
    blocks = devices // BLOCK
    rows_out = BLOCK * small

    wanted = wanted_ref[...]
    need = jnp.max(
        jnp.where(iota((devices, LANES), 1) < 2 * capacity, 0, wanted), axis=0, keepdims=True
    )
    need_ref[...] = jnp.broadcast_to(need, need_ref.shape)
    per_row = LANES // capacity
    halves = []
    for h in range(BLOCK // per_row):
        keys = jnp.zeros((blocks, LANES), jnp.int32)
        for k in range(per_row):
            src = h * per_row + k
            which = wanted_ref[pl.ds(src, blocks, stride=BLOCK), :]
            which = pltpu.roll(which, (k - 1) * capacity % LANES, axis=1)
            which = jnp.where((which > 0) & (which <= small), which + (src * small - 1), -1)
            keys = jnp.where(iota((blocks, LANES), 1) // capacity == k, which, keys)
        halves.append(keys)
    keys = jnp.concatenate(halves, axis=1)
    for b in range(blocks):
        key_ref[b] = keys[b : b + 1, :]

    place = place_ref[...]
    parts = select_ref.shape[1] // LANES
    padded = -(-parts // 8) * 8
    part = place >> 7
    spot = place & (LANES - 1)
    lane = iota((1, LANES), 1)
    left, right = [], []
    for i in range(samples):
        bag = (lane // L * samples + (i + 1)).astype(jnp.float32)
        left.append(ones_where(iota((padded, LANES), 0) == part[i : i + 1, :]))
        right.append(jnp.where(iota((LANES, LANES), 0) == spot[i : i + 1, :], bag, 0.0))
    bags = lax.dot_general(
        jnp.concatenate(left, axis=1).astype(jnp.bfloat16),
        jnp.concatenate(right, axis=1).astype(jnp.bfloat16),
        BOTH_LANES,
        preferred_element_type=jnp.float32,
    ).astype(jnp.int32)
    own = iota((NT * samples, LANES), 0) + 1
    for g in range(parts):
        select_ref[:, g * LANES : (g + 1) * LANES] = ones_where(bags[g : g + 1, :] == own).astype(
            jnp.bfloat16
        )
    base_ref[...] = (
        jnp.dot(
            dense_ref[...],
            wdense_ref[...],
            precision=lax.Precision.HIGHEST,
            preferred_element_type=jnp.float32,
        )
        + bias_ref[...]
    )

    def load(b, hold):
        for k in range(BLOCK):
            for c in range(capacity):
                at = hold + k * capacity + c
                rows_ref[at : at + 1, :] = table_ref[ids_ref[b * BLOCK + k, c]]

    def reduce(b, hold):
        rows = rows_ref[hold : hold + wide, :]
        top = rows.astype(jnp.bfloat16)
        rest = (rows - top.astype(jnp.float32)).astype(jnp.bfloat16)
        gather = ones_where(iota((rows_out, wide), 0) == key_ref[b]).astype(jnp.bfloat16)
        sums = jnp.dot(
            gather, jnp.concatenate([top, rest], axis=1), preferred_element_type=jnp.float32
        )
        start = b * rows_out if isinstance(b, int) else pl.multiple_of(b * rows_out, 8)
        out_ref[pl.ds(start, rows_out), :] = sums[:, :LANES] + sums[:, LANES:]

    if rolled:
        for copy in copies:
            copy.wait()
        lax.fori_loop(0, blocks, lambda b, carry: (load(b, 0), reduce(b, 0), carry)[2], 0)
    else:
        for b in range(blocks):
            if b * BLOCK % chunk == 0:
                copies[b * BLOCK // chunk].wait()
            load(b, b * wide)
            if b >= LAG:
                reduce(b - LAG, (b - LAG) * wide)
        for b in range(blocks - LAG, blocks):
            reduce(b, b * wide)


def pool_kernel(
    rows_ref, select_ref, dense_ref, base_ref, wpair_ref, need_ref,
    pooled_ref, hidden_ref, over_ref,
    *, small,
):
    over_ref[0] = (jnp.max(need_ref[...]) > small).astype(jnp.int32)
    samples = dense_ref.shape[0]
    rows = rows_ref[...]
    top = rows.astype(jnp.bfloat16)
    rest = (rows - top.astype(jnp.float32)).astype(jnp.bfloat16)
    total = jnp.dot(
        select_ref[...],
        jnp.concatenate([top, rest], axis=1),
        preferred_element_type=jnp.float32,
    )
    pooled = total[:, :LANES] + total[:, LANES:]
    feats = [dense_ref[...]] + [pooled[t * samples : (t + 1) * samples] for t in range(NT)]
    for t in range(NT):
        pooled_ref[pl.ds(t, samples, stride=NT), :] = feats[t + 1]
    hidden = base_ref[...]
    k = 0
    for first in range(NT + 1):
        for second in range(first + 1, NT + 1):
            dots = jnp.sum(feats[first] * feats[second], axis=-1, keepdims=True)
            hidden = hidden + dots * wpair_ref[k : k + 1, :]
            k += 1
    hidden_ref[...] = jnp.maximum(hidden, 0.0)


def exchange(
    bag_index, bag_length, emb_tables, dense_feats, w_dense, w_pair, top_bias, *, small, rolled
):
    samples = bag_index.shape[0]
    local_rows = emb_tables.shape[1]
    width = emb_tables.shape[2]
    devices = lax.axis_size("rows") * lax.axis_size("cols")
    capacity = 2 * samples * NT * L // devices
    units = w_dense.shape[1]
    places = devices * small
    vmem = pl.BlockSpec(memory_space=pltpu.VMEM)

    message, place = pl.pallas_call(
        functools.partial(
            route_kernel, local_rows=local_rows, devices=devices, capacity=capacity, small=small
        ),
        out_shape=(
            pltpu.VMEM((devices, LANES), jnp.int32),
            pltpu.VMEM((samples, LANES), jnp.int32),
        ),
        compiler_params=pltpu.CompilerParams(vmem_limit_bytes=16 * 2**20),
        cost_estimate=pl.CostEstimate(flops=10**10, bytes_accessed=10**8, transcendentals=0),
        name="route",
    )(bag_index, bag_length.T)
    wanted = lax.all_to_all(message, ("rows", "cols"), split_axis=0, concat_axis=0, tiled=True)
    found, select, base, need = pl.pallas_call(
        functools.partial(fetch_kernel, capacity=capacity, small=small, rolled=rolled),
        out_shape=(
            pltpu.VMEM((places, width), jnp.float32),
            pltpu.VMEM((samples * NT, places), jnp.bfloat16),
            pltpu.VMEM((samples, units), jnp.float32),
            pltpu.VMEM((8, LANES), jnp.int32),
        ),
        in_specs=[vmem] * 6,
        out_specs=(vmem,) * 4,
        scratch_shapes=[
            pltpu.SMEM((devices, LANES), jnp.int32),
            pltpu.VMEM((devices // BLOCK, 1, BLOCK * capacity), jnp.int32),
            pltpu.VMEM(((BLOCK if rolled else devices) * capacity, width), jnp.float32),
            pltpu.SemaphoreType.DMA((CHUNKS,)),
        ],
        compiler_params=pltpu.CompilerParams(vmem_limit_bytes=(40 if rolled else 16) * 2**20),
        name="fetch",
    )(
        wanted,
        place,
        dense_feats,
        w_dense,
        top_bias.reshape(1, units),
        emb_tables.reshape(NT * local_rows, 1, width),
    )
    fetched = lax.all_to_all(
        found.reshape(places, 1, width),
        ("rows", "cols"),
        split_axis=0,
        concat_axis=0,
        tiled=True,
    )
    return pl.pallas_call(
        functools.partial(pool_kernel, small=small),
        out_shape=(
            jax.ShapeDtypeStruct((samples * NT, width), jnp.float32),
            jax.ShapeDtypeStruct((samples, units), jnp.float32),
            pltpu.SMEM((1,), jnp.int32),
        ),
        in_specs=[vmem] * 6,
        out_specs=(vmem, vmem, pl.BlockSpec(memory_space=pltpu.SMEM)),
        compiler_params=pltpu.CompilerParams(vmem_limit_bytes=16 * 2**20),
        name="pool",
    )(fetched.reshape(places, width), select, dense_feats, base, w_pair, need)


def shards(*args):
    samples = args[0].shape[0]
    capacity = 2 * samples * NT * L // (lax.axis_size("rows") * lax.axis_size("cols"))
    pooled, hidden, over = exchange(*args, small=SMALL, rolled=False)
    args = lax.optimization_barrier((*args, over))[:-1]
    pooled, hidden = lax.switch(
        over[0],
        (lambda p, h: (p, h), lambda p, h: exchange(*args, small=capacity, rolled=True)[:2]),
        pooled,
        hidden,
    )
    return pooled.reshape(samples, NT, -1), hidden


def solution(mesh):
    in_specs = (
        P(("rows", "cols"), None),
        P(("rows", "cols"), None),
        P(None, ("rows", "cols"), None),
        P(("rows", "cols"), None),
        P(),
        P(),
        P(),
    )
    out_specs = (P(("rows", "cols"), None, None), P(("rows", "cols"), None))
    return jax.shard_map(shards, mesh=mesh, in_specs=in_specs, out_specs=out_specs, check_vma=False)
```

```python
import functools

import jax
import jax.numpy as jnp
from jax import lax
from jax.experimental import pallas as pl
from jax.experimental.pallas import tpu as pltpu
from jax.sharding import PartitionSpec as P

NT = 4
L = 32
LANES = 128
SMALL = 25
BLOCK = 8
CHUNKS = 2
LAG = 0
BOTH_LANES = (((1,), (1,)), ((), ()))


def iota(shape, axis):
    return lax.broadcasted_iota(jnp.int32, shape, axis)


def ones_where(mask):
    return jnp.where(mask, 1.0, 0.0)


def route_kernel(idx_ref, len_ref, message_ref, place_ref, *, local_rows, devices, capacity, small):
    samples = idx_ref.shape[0]
    ids = idx_ref[...]
    lane = iota((samples, LANES), 1)
    spread = ones_where(iota((NT, LANES), 1) // L == iota((NT, LANES), 0)).astype(jnp.bfloat16)
    length = lax.dot_general(
        len_ref[...].astype(jnp.float32).astype(jnp.bfloat16),
        spread,
        (((0,), (0,)), ((), ())),
        preferred_element_type=jnp.float32,
    ).astype(jnp.int32)
    target = jnp.where(lane % L < length, ids >> (local_rows.bit_length() - 1), -1)
    code = lane // L * local_rows + (ids & (local_rows - 1))
    high = (code & -256).astype(jnp.float32)
    low = (code & 255).astype(jnp.float32)

    ahead = [
        (pltpu.roll(target, k, axis=1) == target) & (lane % L >= k) for k in range(1, L)
    ]
    repeat = jnp.zeros((samples, LANES), jnp.int32)
    for same in ahead:
        repeat = jnp.where(same, 1, repeat)
    leader = jnp.where(repeat == 0, target, -1)

    owner = iota((devices, LANES), 0)
    row = iota((LANES, LANES), 0)
    column = iota((LANES, LANES), 1)
    earlier = ones_where(row < column).astype(jnp.bfloat16)

    def numbers(targets):
        marks = [ones_where(owner == targets[i : i + 1, :]) for i in range(samples)]
        seen = marks[0]
        for mark in marks[1:]:
            seen = seen + mark
        running = jnp.dot(
            seen.astype(jnp.bfloat16), earlier, preferred_element_type=jnp.float32
        )
        found = []
        for mark in marks:
            found.append(jnp.sum(mark * running, axis=0, keepdims=True))
            running = running + mark
        return marks, found, seen

    hots, ranks, _ = numbers(target)
    _, orders, seen = numbers(leader)
    order = jnp.concatenate(orders, axis=0)
    which = order
    for k, same in enumerate(ahead, 1):
        lead = pltpu.roll(leader, k, axis=1) >= 0
        which = jnp.where(same & lead, pltpu.roll(order, k, axis=1), which)
    which = which + 1.0
    slot = iota((capacity, LANES), 0).astype(jnp.float32)
    pieces = []
    for i in range(samples):
        here = slot == ranks[i]
        pieces.append(
            jnp.concatenate(
                [
                    jnp.where(here, value[i : i + 1, :], 0.0)
                    for value in (high, which, low)
                ]
                + [jnp.zeros((LANES - 3 * capacity, LANES), jnp.float32)],
                axis=0,
            ).astype(jnp.bfloat16)
        )
    number = which.astype(jnp.int32)
    place_ref[...] = jnp.where(
        (leader >= 0) & (number <= small), target * small + number - 1, -1
    )
    hot_wide = jnp.concatenate([h.astype(jnp.bfloat16) for h in hots], axis=1)
    box = lax.dot_general(
        hot_wide,
        jnp.concatenate(pieces, axis=1),
        BOTH_LANES,
        preferred_element_type=jnp.float32,
    )
    side = iota((devices, LANES), 1)
    box = box + jnp.where(
        side < capacity, pltpu.roll(box, LANES - 2 * capacity, axis=1), 0.0
    )
    need = jnp.max(jnp.sum(seen, axis=1, keepdims=True), axis=0, keepdims=True)
    message_ref[...] = jnp.where(
        side < 2 * capacity, box, need
    ).astype(jnp.int32)


def fetch_kernel(
    wanted_ref, place_ref, dense_ref, wdense_ref, bias_ref, table_ref,
    out_ref, select_ref, base_ref, need_ref, ids_ref, key_ref, rows_ref, sems,
    *, capacity, small, rolled,
):
    devices = wanted_ref.shape[0]
    chunk = devices // CHUNKS
    copies = [
        pltpu.make_async_copy(
            wanted_ref.at[pl.ds(k * chunk, chunk)], ids_ref.at[pl.ds(k * chunk, chunk)], sems.at[k]
        )
        for k in range(CHUNKS)
    ]
    for copy in copies:
        copy.start()
    samples = place_ref.shape[0]
    wide = BLOCK * capacity
    blocks = devices // BLOCK
    rows_out = BLOCK * small

    wanted = wanted_ref[...]
    need = jnp.max(
        jnp.where(iota((devices, LANES), 1) < 2 * capacity, 0, wanted), axis=0, keepdims=True
    )
    need_ref[...] = jnp.broadcast_to(need, need_ref.shape)
    per_row = LANES // capacity
    halves = []
    for h in range(BLOCK // per_row):
        keys = jnp.zeros((blocks, LANES), jnp.int32)
        for k in range(per_row):
            src = h * per_row + k
            which = wanted_ref[pl.ds(src, blocks, stride=BLOCK), :]
            which = pltpu.roll(which, (k - 1) * capacity % LANES, axis=1)
            which = jnp.where((which > 0) & (which <= small), which + (src * small - 1), -1)
            keys = jnp.where(iota((blocks, LANES), 1) // capacity == k, which, keys)
        halves.append(keys)
    keys = jnp.concatenate(halves, axis=1)
    for b in range(blocks):
        key_ref[b] = keys[b : b + 1, :]

    place = place_ref[...]
    parts = select_ref.shape[1] // LANES
    padded = -(-parts // 8) * 8
    part = place >> 7
    spot = place & (LANES - 1)
    lane = iota((1, LANES), 1)
    left, right = [], []
    for i in range(samples):
        bag = (lane // L * samples + (i + 1)).astype(jnp.float32)
        left.append(ones_where(iota((padded, LANES), 0) == part[i : i + 1, :]))
        right.append(jnp.where(iota((LANES, LANES), 0) == spot[i : i + 1, :], bag, 0.0))
    bags = lax.dot_general(
        jnp.concatenate(left, axis=1).astype(jnp.bfloat16),
        jnp.concatenate(right, axis=1).astype(jnp.bfloat16),
        BOTH_LANES,
        preferred_element_type=jnp.float32,
    ).astype(jnp.int32)
    own = iota((NT * samples, LANES), 0) + 1
    for g in range(parts):
        select_ref[:, g * LANES : (g + 1) * LANES] = ones_where(bags[g : g + 1, :] == own).astype(
            jnp.bfloat16
        )
    base_ref[...] = (
        jnp.dot(
            dense_ref[...],
            wdense_ref[...],
            precision=lax.Precision.HIGHEST,
            preferred_element_type=jnp.float32,
        )
        + bias_ref[...]
    )

    def load(b, hold):
        for k in range(BLOCK):
            for c in range(capacity):
                at = hold + k * capacity + c
                rows_ref[at : at + 1, :] = table_ref[ids_ref[b * BLOCK + k, c]]

    def reduce(b, hold):
        rows = rows_ref[hold : hold + wide, :]
        top = rows.astype(jnp.bfloat16)
        rest = (rows - top.astype(jnp.float32)).astype(jnp.bfloat16)
        gather = ones_where(iota((rows_out, wide), 0) == key_ref[b]).astype(jnp.bfloat16)
        sums = jnp.dot(
            gather, jnp.concatenate([top, rest], axis=1), preferred_element_type=jnp.float32
        )
        start = b * rows_out if isinstance(b, int) else pl.multiple_of(b * rows_out, 8)
        out_ref[pl.ds(start, rows_out), :] = sums[:, :LANES] + sums[:, LANES:]

    if rolled:
        for copy in copies:
            copy.wait()
        lax.fori_loop(0, blocks, lambda b, carry: (load(b, 0), reduce(b, 0), carry)[2], 0)
    else:
        for b in range(blocks):
            if b * BLOCK % chunk == 0:
                copies[b * BLOCK // chunk].wait()
            load(b, b * wide)
            if b >= LAG:
                reduce(b - LAG, (b - LAG) * wide)
        for b in range(blocks - LAG, blocks):
            reduce(b, b * wide)


def pool_kernel(
    rows_ref, select_ref, dense_ref, base_ref, wpair_ref, need_ref,
    pooled_ref, hidden_ref, over_ref,
    *, small,
):
    over_ref[0] = (jnp.max(need_ref[...]) > small).astype(jnp.int32)
    samples = dense_ref.shape[0]
    rows = rows_ref[...]
    top = rows.astype(jnp.bfloat16)
    rest = (rows - top.astype(jnp.float32)).astype(jnp.bfloat16)
    total = jnp.dot(
        select_ref[...],
        jnp.concatenate([top, rest], axis=1),
        preferred_element_type=jnp.float32,
    )
    pooled = total[:, :LANES] + total[:, LANES:]
    feats = [dense_ref[...]] + [pooled[t * samples : (t + 1) * samples] for t in range(NT)]
    for t in range(NT):
        pooled_ref[pl.ds(t, samples, stride=NT), :] = feats[t + 1]
    hidden = base_ref[...]
    k = 0
    for first in range(NT + 1):
        for second in range(first + 1, NT + 1):
            dots = jnp.sum(feats[first] * feats[second], axis=-1, keepdims=True)
            hidden = hidden + dots * wpair_ref[k : k + 1, :]
            k += 1
    hidden_ref[...] = jnp.maximum(hidden, 0.0)


def exchange(
    bag_index, bag_length, emb_tables, dense_feats, w_dense, w_pair, top_bias, *, small, rolled
):
    samples = bag_index.shape[0]
    local_rows = emb_tables.shape[1]
    width = emb_tables.shape[2]
    devices = lax.axis_size("rows") * lax.axis_size("cols")
    capacity = 2 * samples * NT * L // devices
    units = w_dense.shape[1]
    places = devices * small
    vmem = pl.BlockSpec(memory_space=pltpu.VMEM)

    message, place = pl.pallas_call(
        functools.partial(
            route_kernel, local_rows=local_rows, devices=devices, capacity=capacity, small=small
        ),
        out_shape=(
            pltpu.VMEM((devices, LANES), jnp.int32),
            pltpu.VMEM((samples, LANES), jnp.int32),
        ),
        compiler_params=pltpu.CompilerParams(vmem_limit_bytes=16 * 2**20),
        cost_estimate=pl.CostEstimate(flops=10**10, bytes_accessed=10**8, transcendentals=0),
        name="route",
    )(bag_index, bag_length.T)
    wanted = lax.all_to_all(message, ("rows", "cols"), split_axis=0, concat_axis=0, tiled=True)
    found, select, base, need = pl.pallas_call(
        functools.partial(fetch_kernel, capacity=capacity, small=small, rolled=rolled),
        out_shape=(
            pltpu.VMEM((places, width), jnp.float32),
            pltpu.VMEM((samples * NT, places), jnp.bfloat16),
            pltpu.VMEM((samples, units), jnp.float32),
            pltpu.VMEM((8, LANES), jnp.int32),
        ),
        in_specs=[vmem] * 6,
        out_specs=(vmem,) * 4,
        scratch_shapes=[
            pltpu.SMEM((devices, LANES), jnp.int32),
            pltpu.VMEM((devices // BLOCK, 1, BLOCK * capacity), jnp.int32),
            pltpu.VMEM(((BLOCK if rolled else devices) * capacity, width), jnp.float32),
            pltpu.SemaphoreType.DMA((CHUNKS,)),
        ],
        compiler_params=pltpu.CompilerParams(vmem_limit_bytes=(40 if rolled else 16) * 2**20),
        name="fetch",
    )(
        wanted,
        place,
        dense_feats,
        w_dense,
        top_bias.reshape(1, units),
        emb_tables.reshape(NT * local_rows, 1, width),
    )
    fetched = lax.all_to_all(
        found.reshape(places, 1, width),
        ("rows", "cols"),
        split_axis=0,
        concat_axis=0,
        tiled=True,
    )
    return pl.pallas_call(
        functools.partial(pool_kernel, small=small),
        out_shape=(
            jax.ShapeDtypeStruct((samples * NT, width), jnp.float32),
            jax.ShapeDtypeStruct((samples, units), jnp.float32),
            pltpu.SMEM((1,), jnp.int32),
        ),
        in_specs=[vmem] * 6,
        out_specs=(vmem, vmem, pl.BlockSpec(memory_space=pltpu.SMEM)),
        compiler_params=pltpu.CompilerParams(vmem_limit_bytes=16 * 2**20),
        name="pool",
    )(fetched.reshape(places, width), select, dense_feats, base, w_pair, need)


def shards(*args):
    samples = args[0].shape[0]
    capacity = 2 * samples * NT * L // (lax.axis_size("rows") * lax.axis_size("cols"))
    pooled, hidden, over = exchange(*args, small=SMALL, rolled=False)
    args = lax.optimization_barrier((*args, over))[:-1]
    pooled, hidden = lax.switch(
        over[0],
        (lambda p, h: (p, h), lambda p, h: exchange(*args, small=capacity, rolled=True)[:2]),
        pooled,
        hidden,
    )
    return pooled.reshape(samples, NT, -1), hidden


def solution(mesh):
    in_specs = (
        P(("rows", "cols"), None),
        P(("rows", "cols"), None),
        P(None, ("rows", "cols"), None),
        P(("rows", "cols"), None),
        P(),
        P(),
        P(),
    )
    out_specs = (P(("rows", "cols"), None, None), P(("rows", "cols"), None))
    return jax.shard_map(shards, mesh=mesh, in_specs=in_specs, out_specs=out_specs, check_vma=False)
```

```python
import functools

import jax
import jax.numpy as jnp
from jax import lax
from jax.experimental import pallas as pl
from jax.experimental.pallas import tpu as pltpu
from jax.sharding import PartitionSpec as P

NT = 4
L = 32
LANES = 128
SMALL = 25
BLOCK = 8
CHUNKS = 3
LAG = 0
BOTH_LANES = (((1,), (1,)), ((), ()))


def iota(shape, axis):
    return lax.broadcasted_iota(jnp.int32, shape, axis)


def ones_where(mask):
    return jnp.where(mask, 1.0, 0.0)


def route_kernel(idx_ref, len_ref, message_ref, place_ref, *, local_rows, devices, capacity, small):
    samples = idx_ref.shape[0]
    ids = idx_ref[...]
    lane = iota((samples, LANES), 1)
    spread = ones_where(iota((NT, LANES), 1) // L == iota((NT, LANES), 0)).astype(jnp.bfloat16)
    length = lax.dot_general(
        len_ref[...].astype(jnp.float32).astype(jnp.bfloat16),
        spread,
        (((0,), (0,)), ((), ())),
        preferred_element_type=jnp.float32,
    ).astype(jnp.int32)
    target = jnp.where(lane % L < length, ids >> (local_rows.bit_length() - 1), -1)
    code = lane // L * local_rows + (ids & (local_rows - 1))
    high = (code & -256).astype(jnp.float32)
    low = (code & 255).astype(jnp.float32)

    ahead = [
        (pltpu.roll(target, k, axis=1) == target) & (lane % L >= k) for k in range(1, L)
    ]
    repeat = jnp.zeros((samples, LANES), jnp.int32)
    for same in ahead:
        repeat = jnp.where(same, 1, repeat)
    leader = jnp.where(repeat == 0, target, -1)

    owner = iota((devices, LANES), 0)
    row = iota((LANES, LANES), 0)
    column = iota((LANES, LANES), 1)
    earlier = ones_where(row < column).astype(jnp.bfloat16)

    def numbers(targets):
        marks = [ones_where(owner == targets[i : i + 1, :]) for i in range(samples)]
        seen = marks[0]
        for mark in marks[1:]:
            seen = seen + mark
        running = jnp.dot(
            seen.astype(jnp.bfloat16), earlier, preferred_element_type=jnp.float32
        )
        found = []
        for mark in marks:
            found.append(jnp.sum(mark * running, axis=0, keepdims=True))
            running = running + mark
        return marks, found, seen

    hots, ranks, _ = numbers(target)
    _, orders, seen = numbers(leader)
    order = jnp.concatenate(orders, axis=0)
    which = order
    for k, same in enumerate(ahead, 1):
        lead = pltpu.roll(leader, k, axis=1) >= 0
        which = jnp.where(same & lead, pltpu.roll(order, k, axis=1), which)
    which = which + 1.0
    slot = iota((capacity, LANES), 0).astype(jnp.float32)
    pieces = []
    for i in range(samples):
        here = slot == ranks[i]
        pieces.append(
            jnp.concatenate(
                [
                    jnp.where(here, value[i : i + 1, :], 0.0)
                    for value in (high, which, low)
                ]
                + [jnp.zeros((LANES - 3 * capacity, LANES), jnp.float32)],
                axis=0,
            ).astype(jnp.bfloat16)
        )
    number = which.astype(jnp.int32)
    place_ref[...] = jnp.where(
        (leader >= 0) & (number <= small), target * small + number - 1, -1
    )
    hot_wide = jnp.concatenate([h.astype(jnp.bfloat16) for h in hots], axis=1)
    box = lax.dot_general(
        hot_wide,
        jnp.concatenate(pieces, axis=1),
        BOTH_LANES,
        preferred_element_type=jnp.float32,
    )
    side = iota((devices, LANES), 1)
    box = box + jnp.where(
        side < capacity, pltpu.roll(box, LANES - 2 * capacity, axis=1), 0.0
    )
    need = jnp.max(jnp.sum(seen, axis=1, keepdims=True), axis=0, keepdims=True)
    message_ref[...] = jnp.where(
        side < 2 * capacity, box, need
    ).astype(jnp.int32)


def fetch_kernel(
    wanted_ref, place_ref, dense_ref, wdense_ref, bias_ref, table_ref,
    out_ref, select_ref, base_ref, need_ref, ids_ref, key_ref, rows_ref, sems,
    *, capacity, small, rolled,
):
    devices = wanted_ref.shape[0]
    starts = (0, 2 * BLOCK, devices // 2, devices)
    copies = [
        pltpu.make_async_copy(
            wanted_ref.at[pl.ds(start, end - start)], ids_ref.at[pl.ds(start, end - start)], sems.at[k]
        )
        for k, (start, end) in enumerate(zip(starts, starts[1:]))
    ]
    for copy in copies:
        copy.start()
    samples = place_ref.shape[0]
    wide = BLOCK * capacity
    blocks = devices // BLOCK
    rows_out = BLOCK * small

    wanted = wanted_ref[...]
    need = jnp.max(
        jnp.where(iota((devices, LANES), 1) < 2 * capacity, 0, wanted), axis=0, keepdims=True
    )
    need_ref[...] = jnp.broadcast_to(need, need_ref.shape)
    per_row = LANES // capacity
    halves = []
    for h in range(BLOCK // per_row):
        keys = jnp.zeros((blocks, LANES), jnp.int32)
        for k in range(per_row):
            src = h * per_row + k
            which = wanted_ref[pl.ds(src, blocks, stride=BLOCK), :]
            which = pltpu.roll(which, (k - 1) * capacity % LANES, axis=1)
            which = jnp.where((which > 0) & (which <= small), which + (src * small - 1), -1)
            keys = jnp.where(iota((blocks, LANES), 1) // capacity == k, which, keys)
        halves.append(keys)
    keys = jnp.concatenate(halves, axis=1)
    for b in range(blocks):
        key_ref[b] = keys[b : b + 1, :]

    place = place_ref[...]
    parts = select_ref.shape[1] // LANES
    padded = -(-parts // 8) * 8
    part = place >> 7
    spot = place & (LANES - 1)
    lane = iota((1, LANES), 1)
    left, right = [], []
    for i in range(samples):
        bag = (lane // L * samples + (i + 1)).astype(jnp.float32)
        left.append(ones_where(iota((padded, LANES), 0) == part[i : i + 1, :]))
        right.append(jnp.where(iota((LANES, LANES), 0) == spot[i : i + 1, :], bag, 0.0))
    bags = lax.dot_general(
        jnp.concatenate(left, axis=1).astype(jnp.bfloat16),
        jnp.concatenate(right, axis=1).astype(jnp.bfloat16),
        BOTH_LANES,
        preferred_element_type=jnp.float32,
    ).astype(jnp.int32)
    own = iota((NT * samples, LANES), 0) + 1
    for g in range(parts):
        select_ref[:, g * LANES : (g + 1) * LANES] = ones_where(bags[g : g + 1, :] == own).astype(
            jnp.bfloat16
        )
    base_ref[...] = (
        jnp.dot(
            dense_ref[...],
            wdense_ref[...],
            precision=lax.Precision.HIGHEST,
            preferred_element_type=jnp.float32,
        )
        + bias_ref[...]
    )

    def load(b, hold):
        for k in range(BLOCK):
            for c in range(capacity):
                at = hold + k * capacity + c
                rows_ref[at : at + 1, :] = table_ref[ids_ref[b * BLOCK + k, c]]

    def reduce(b, hold):
        rows = rows_ref[hold : hold + wide, :]
        top = rows.astype(jnp.bfloat16)
        rest = (rows - top.astype(jnp.float32)).astype(jnp.bfloat16)
        gather = ones_where(iota((rows_out, wide), 0) == key_ref[b]).astype(jnp.bfloat16)
        sums = jnp.dot(
            gather, jnp.concatenate([top, rest], axis=1), preferred_element_type=jnp.float32
        )
        start = b * rows_out if isinstance(b, int) else pl.multiple_of(b * rows_out, 8)
        out_ref[pl.ds(start, rows_out), :] = sums[:, :LANES] + sums[:, LANES:]

    if rolled:
        for copy in copies:
            copy.wait()
        lax.fori_loop(0, blocks, lambda b, carry: (load(b, 0), reduce(b, 0), carry)[2], 0)
    else:
        for b in range(blocks):
            if b * BLOCK in starts:
                copies[starts.index(b * BLOCK)].wait()
            load(b, b * wide)
            if b >= LAG:
                reduce(b - LAG, (b - LAG) * wide)
        for b in range(blocks - LAG, blocks):
            reduce(b, b * wide)


def pool_kernel(
    rows_ref, select_ref, dense_ref, base_ref, wpair_ref, need_ref,
    pooled_ref, hidden_ref, over_ref,
    *, small,
):
    over_ref[0] = (jnp.max(need_ref[...]) > small).astype(jnp.int32)
    samples = dense_ref.shape[0]
    rows = rows_ref[...]
    top = rows.astype(jnp.bfloat16)
    rest = (rows - top.astype(jnp.float32)).astype(jnp.bfloat16)
    total = jnp.dot(
        select_ref[...],
        jnp.concatenate([top, rest], axis=1),
        preferred_element_type=jnp.float32,
    )
    pooled = total[:, :LANES] + total[:, LANES:]
    feats = [dense_ref[...]] + [pooled[t * samples : (t + 1) * samples] for t in range(NT)]
    for t in range(NT):
        pooled_ref[pl.ds(t, samples, stride=NT), :] = feats[t + 1]
    hidden = base_ref[...]
    k = 0
    for first in range(NT + 1):
        for second in range(first + 1, NT + 1):
            dots = jnp.sum(feats[first] * feats[second], axis=-1, keepdims=True)
            hidden = hidden + dots * wpair_ref[k : k + 1, :]
            k += 1
    hidden_ref[...] = jnp.maximum(hidden, 0.0)


def exchange(
    bag_index, bag_length, emb_tables, dense_feats, w_dense, w_pair, top_bias, *, small, rolled
):
    samples = bag_index.shape[0]
    local_rows = emb_tables.shape[1]
    width = emb_tables.shape[2]
    devices = lax.axis_size("rows") * lax.axis_size("cols")
    capacity = 2 * samples * NT * L // devices
    units = w_dense.shape[1]
    places = devices * small
    vmem = pl.BlockSpec(memory_space=pltpu.VMEM)

    message, place = pl.pallas_call(
        functools.partial(
            route_kernel, local_rows=local_rows, devices=devices, capacity=capacity, small=small
        ),
        out_shape=(
            pltpu.VMEM((devices, LANES), jnp.int32),
            pltpu.VMEM((samples, LANES), jnp.int32),
        ),
        compiler_params=pltpu.CompilerParams(vmem_limit_bytes=16 * 2**20),
        cost_estimate=pl.CostEstimate(flops=10**10, bytes_accessed=10**8, transcendentals=0),
        name="route",
    )(bag_index, bag_length.T)
    wanted = lax.all_to_all(message, ("rows", "cols"), split_axis=0, concat_axis=0, tiled=True)
    found, select, base, need = pl.pallas_call(
        functools.partial(fetch_kernel, capacity=capacity, small=small, rolled=rolled),
        out_shape=(
            pltpu.VMEM((places, width), jnp.float32),
            pltpu.VMEM((samples * NT, places), jnp.bfloat16),
            pltpu.VMEM((samples, units), jnp.float32),
            pltpu.VMEM((8, LANES), jnp.int32),
        ),
        in_specs=[vmem] * 6,
        out_specs=(vmem,) * 4,
        scratch_shapes=[
            pltpu.SMEM((devices, LANES), jnp.int32),
            pltpu.VMEM((devices // BLOCK, 1, BLOCK * capacity), jnp.int32),
            pltpu.VMEM(((BLOCK if rolled else devices) * capacity, width), jnp.float32),
            pltpu.SemaphoreType.DMA((CHUNKS,)),
        ],
        compiler_params=pltpu.CompilerParams(vmem_limit_bytes=(40 if rolled else 16) * 2**20),
        name="fetch",
    )(
        wanted,
        place,
        dense_feats,
        w_dense,
        top_bias.reshape(1, units),
        emb_tables.reshape(NT * local_rows, 1, width),
    )
    fetched = lax.all_to_all(
        found.reshape(places, 1, width),
        ("rows", "cols"),
        split_axis=0,
        concat_axis=0,
        tiled=True,
    )
    return pl.pallas_call(
        functools.partial(pool_kernel, small=small),
        out_shape=(
            jax.ShapeDtypeStruct((samples * NT, width), jnp.float32),
            jax.ShapeDtypeStruct((samples, units), jnp.float32),
            pltpu.SMEM((1,), jnp.int32),
        ),
        in_specs=[vmem] * 6,
        out_specs=(vmem, vmem, pl.BlockSpec(memory_space=pltpu.SMEM)),
        compiler_params=pltpu.CompilerParams(vmem_limit_bytes=16 * 2**20),
        name="pool",
    )(fetched.reshape(places, width), select, dense_feats, base, w_pair, need)


def shards(*args):
    samples = args[0].shape[0]
    capacity = 2 * samples * NT * L // (lax.axis_size("rows") * lax.axis_size("cols"))
    pooled, hidden, over = exchange(*args, small=SMALL, rolled=False)
    args = lax.optimization_barrier((*args, over))[:-1]
    pooled, hidden = lax.switch(
        over[0],
        (lambda p, h: (p, h), lambda p, h: exchange(*args, small=capacity, rolled=True)[:2]),
        pooled,
        hidden,
    )
    return pooled.reshape(samples, NT, -1), hidden


def solution(mesh):
    in_specs = (
        P(("rows", "cols"), None),
        P(("rows", "cols"), None),
        P(None, ("rows", "cols"), None),
        P(("rows", "cols"), None),
        P(),
        P(),
        P(),
    )
    out_specs = (P(("rows", "cols"), None, None), P(("rows", "cols"), None))
    return jax.shard_map(shards, mesh=mesh, in_specs=in_specs, out_specs=out_specs, check_vma=False)
```
